8 devices in a mesh: data: 8 (over z, y, x, core).
Axes of the slice: x: 2, y: 2, z: 1, core: 2. Of those that a mesh axis runs over, the one named last changes fastest.
Arguments:
- tokens: bfloat16 [4096, 1024], P('data')
- labels: int32 [3, 4096], P(None, 'data')
- w_one: bfloat16 [1024, 4096], replicated
- w_two: bfloat16 [4096, 1024], replicated
- adapter_a: bfloat16 [1024, 8], replicated
- adapter_b: bfloat16 [8, 4096], replicated
- task_heads: bfloat16 [3, 1024, 3], replicated
Outputs:
- output 1: float32 [3], replicated
- output 2: float32 [1024, 8], P('data')
- output 3: float32 [8, 4096], P(None, 'data')
All inputs are finite; a program needn't handle non-finite values.
Results may differ from the reference program's by a relative error of at most 0.00122422.
Values are sent between devices in bfloat16 or wider.
A program may use at most 1 GiB of HBM per device.

```python
import jax
import jax.numpy as jnp
from jax import lax

DEVICES = 8
TOK_DEV = 512
D_MODEL = 1024
D_FF = 4096
LORA_RANK = 8
NUM_TASKS = 3
NUM_CLASSES = 3
EG_STEPS = 20


def draw_labels(label_key):
    key_list = jax.random.split(label_key, 4)
    total_tok = DEVICES * TOK_DEV
    dev_shift = jax.random.randint(key_list[0], (DEVICES, 1), 0, NUM_CLASSES)
    half_width = (NUM_CLASSES + 1) // 2
    common_lab = (dev_shift + jax.random.randint(key_list[1], (DEVICES, TOK_DEV), 0, half_width)) % NUM_CLASSES
    common_lab = common_lab.reshape(total_tok)
    own_lab = jax.random.randint(key_list[2], (NUM_TASKS, total_tok), 0, NUM_CLASSES)
    pick_common = jax.random.randint(key_list[3], (NUM_TASKS, total_tok), 0, 5) < 3
    return jnp.where(pick_common, common_lab[None, :], own_lab).astype(jnp.int32)


def setup_inputs(seed: int = 0) -> dict:
    key_list = jax.random.split(jax.random.key(seed), 8)
    total_tok = DEVICES * TOK_DEV
    tokens = jax.random.normal(key_list[0], (total_tok, D_MODEL), jnp.float32)
    w_one = jax.random.normal(key_list[1], (D_MODEL, D_FF), jnp.float32) * D_MODEL ** -0.5
    w_two = jax.random.normal(key_list[2], (D_FF, D_MODEL), jnp.float32) * D_FF ** -0.5
    adapter_a = jax.random.normal(key_list[3], (D_MODEL, LORA_RANK), jnp.float32) * D_MODEL ** -0.5
    adapter_b = jax.random.normal(key_list[4], (LORA_RANK, D_FF), jnp.float32) * LORA_RANK ** -0.5
    head_common = jax.random.normal(key_list[5], (D_MODEL, NUM_CLASSES), jnp.float32)
    head_own = jax.random.normal(key_list[6], (NUM_TASKS, D_MODEL, NUM_CLASSES), jnp.float32)
    head_sign = jnp.where(jnp.arange(NUM_TASKS) % 2 == 0, 1.0, -1.0)
    task_heads = (head_sign[:, None, None] * head_common[None] + 0.8 * head_own) * (1.5 * D_MODEL ** -0.5)
    labels = draw_labels(key_list[7])
    return {
        "tokens": tokens.astype(jnp.bfloat16),
        "labels": labels,
        "w_one": w_one.astype(jnp.bfloat16),
        "w_two": w_two.astype(jnp.bfloat16),
        "adapter_a": adapter_a.astype(jnp.bfloat16),
        "adapter_b": adapter_b.astype(jnp.bfloat16),
        "task_heads": task_heads.astype(jnp.bfloat16),
    }


def block_grads(tok_blk, lab_blk, w_one, w_two, adapter_a, adapter_b, task_heads):
    low_rank = jnp.dot(tok_blk, adapter_a, preferred_element_type=jnp.float32).astype(jnp.bfloat16)
    pre_act = jnp.dot(tok_blk, w_one, preferred_element_type=jnp.float32) + jnp.dot(low_rank, adapter_b, preferred_element_type=jnp.float32)
    gelu_out, gelu_slope = jax.jvp(jax.nn.gelu, (pre_act,), (jnp.ones_like(pre_act),))
    hidden = gelu_out.astype(jnp.bfloat16)
    trunk_out = (tok_blk.astype(jnp.float32) + jnp.dot(hidden, w_two, preferred_element_type=jnp.float32)).astype(jnp.bfloat16)
    logits = jnp.einsum("bd,tdc->tbc", trunk_out.astype(jnp.float32), task_heads.astype(jnp.float32))
    task_probs = jax.nn.softmax(logits, axis=-1)
    onehot = (lab_blk[:, :, None] == jnp.arange(NUM_CLASSES)[None, None, :]).astype(jnp.float32)
    logit_err = (task_probs - onehot).astype(jnp.bfloat16)
    d_trunk = jnp.einsum("tbc,tdc->tbd", logit_err.astype(jnp.float32), task_heads.astype(jnp.float32)).astype(jnp.bfloat16)
    d_hidden = jnp.einsum("tbd,fd->tbf", d_trunk.astype(jnp.float32), w_two.astype(jnp.float32))
    d_pre = (d_hidden * gelu_slope[None]).astype(jnp.bfloat16)
    part_b = jnp.einsum("br,tbf->trf", low_rank.astype(jnp.float32), d_pre.astype(jnp.float32))
    d_low = jnp.einsum("tbf,rf->tbr", d_pre.astype(jnp.float32), adapter_b.astype(jnp.float32)).astype(jnp.bfloat16)
    part_a = jnp.einsum("bd,tbr->tdr", tok_blk.astype(jnp.float32), d_low.astype(jnp.float32))
    return part_a, part_b


def reference(tokens, labels, w_one, w_two, adapter_a, adapter_b, task_heads):
    tok_blocks = tokens.reshape(DEVICES, TOK_DEV, D_MODEL)
    lab_blocks = labels.reshape(NUM_TASKS, DEVICES, TOK_DEV).transpose(1, 0, 2)

    def add_block(run_sum, block_in):
        part_a, part_b = block_grads(block_in[0], block_in[1], w_one, w_two, adapter_a, adapter_b, task_heads)
        return (run_sum[0] + part_a, run_sum[1] + part_b), None

    zero_init = (jnp.zeros((NUM_TASKS, D_MODEL, LORA_RANK), jnp.float32), jnp.zeros((NUM_TASKS, LORA_RANK, D_FF), jnp.float32))
    sums, _ = lax.scan(add_block, zero_init, (tok_blocks, lab_blocks))
    batch_total = DEVICES * TOK_DEV
    grad_a = sums[0] / batch_total
    grad_b = sums[1] / batch_total
    gram_mat = jnp.einsum("tdr,sdr->ts", grad_a, grad_a) + jnp.einsum("trf,srf->ts", grad_b, grad_b)
    eg_scale = jnp.trace(gram_mat) / NUM_TASKS

    def eg_step(weights, _):
        weights = weights * jnp.exp(-jnp.sum(gram_mat * weights[None, :], axis=1) / eg_scale)
        return weights / jnp.sum(weights), None

    task_weights, _ = lax.scan(eg_step, jnp.full((NUM_TASKS,), 1.0 / NUM_TASKS, jnp.float32), None, length=EG_STEPS)
    comb_a = jnp.sum(task_weights[:, None, None] * grad_a, axis=0)
    comb_b = jnp.sum(task_weights[:, None, None] * grad_b, axis=0)
    return (task_weights, comb_a, comb_b)
```

```python
import functools

import jax
import jax.numpy as jnp
import numpy as np
from jax import lax
from jax.experimental import pallas as pl
from jax.experimental.pallas import tpu as pltpu
from jax.sharding import PartitionSpec as P

EG_STEPS = 20
MESH = pl.DeviceIdType.MESH
F32, BF16 = jnp.float32, jnp.bfloat16
GELU_C = float(np.sqrt(2.0 / np.pi))
GELU_A = 0.044715
NT = (((1,), (1,)), ((), ()))


def dot(lhs, rhs):
    return jnp.dot(lhs, rhs, preferred_element_type=F32)


def dot_nt(lhs, rhs):
    return lax.dot_general(lhs, rhs, NT, preferred_element_type=F32)


def fused_kernel(ndev, batch_total, x_hbm, lab_hbm, w1_hbm, w2_hbm, at_hbm, bm_hbm, ht_hbm,
                 alpha_ref, ga_ref, gb_ref,
                 xs, w1s, w2s, ats, bms, hts_in, labs, uts, us, p_a, p_b, h_a, h_b, slope, zacc, zs,
                 hfs, hrow, hcat, dzs, dp_a, dp_b, dlacc, gbs, gbr, gas, gar, ms, mr,
                 w1sem, w2sem, insem, gb_ss, gb_rs, ga_ss, ga_rs, m_ss, m_rs):
    tok = xs.shape[0]
    dff = w2_hbm.shape[0]
    fb = dff // ndev
    rank = ats.shape[0]
    tasks = hts_in.shape[0]
    ncls = hts_in.shape[1]
    dm = xs.shape[1]
    own = dm // ndev
    me = lax.axis_index("data")

    barrier = pltpu.get_barrier_semaphore()
    for off in range(1, ndev):
        pl.semaphore_signal(barrier, inc=1, device_id=(lax.rem(me + off, ndev),), device_id_type=MESH)

    def small(i):
        pairs = [(at_hbm, ats), (x_hbm, xs), (bm_hbm, bms), (ht_hbm, hts_in), (lab_hbm, labs)]
        return pltpu.make_async_copy(pairs[i][0], pairs[i][1], insem.at[i])

    def w1_copy(j):
        return pltpu.make_async_copy(w1_hbm.at[:, pl.ds(pl.multiple_of(j * fb, fb), fb)], w1s.at[j], w1sem.at[j])

    def w2_copy(j):
        return pltpu.make_async_copy(w2_hbm.at[pl.ds(pl.multiple_of(j * fb, fb), fb), :], w2s.at[j], w2sem.at[j])

    for i in range(3):
        small(i).start()
    w1_copy(0).start()
    w1_copy(1).start()
    w2_copy(0).start()
    small(3).start()
    small(4).start()
    for j in range(2, ndev):
        w1_copy(j).start()
        w2_copy(j - 1).start()
    w2_copy(ndev - 1).start()

    small(0).wait()
    small(1).wait()
    ut = dot_nt(ats[...], xs[...])
    uts[...] = ut.astype(BF16)
    us[...] = ut.T.astype(BF16)
    small(2).wait()
    zacc[...] = jnp.zeros_like(zacc)
    dlacc[...] = jnp.zeros_like(dlacc)
    hfs[...] = jnp.zeros_like(hfs)

    def block_of(ref, j):
        return ref[:, pl.ds(pl.multiple_of(j * fb, fb), fb)]

    def fwd_in(j, p_ref):
        w1_copy(j).wait()
        p_ref[...] = dot(xs[...], w1s[j]) + dot(us[...], block_of(bms, j))

    def fwd_act(j, p_ref, h_ref):
        x = p_ref[...]
        x2 = x * x
        t = jnp.tanh(x * (GELU_C + (GELU_C * GELU_A) * x2))
        cdf = 0.5 + 0.5 * t
        h_ref[...] = (x * cdf).astype(BF16)
        w = cdf * (1.0 - cdf)
        slope[j] = cdf + x * (w * (2.0 * GELU_C + (6.0 * GELU_C * GELU_A) * x2))

    def fwd_out(j, h_ref):
        w2_copy(j).wait()
        zacc[...] += dot(h_ref[...], w2s[j])

    ps, hs = (p_a, p_b), (h_a, h_b)
    fwd_in(0, p_a)
    fwd_in(1, p_b)
    fwd_act(0, p_a, h_a)

    def fwd_pair(i, carry):
        for k in range(2):
            j = 2 * i + k
            fwd_in(j + 2, ps[k])
            fwd_act(j + 1, ps[1 - k], hs[1 - k])
            fwd_out(j, hs[k])
        return carry

    lax.fori_loop(0, (ndev - 2) // 2, fwd_pair, 0)
    fwd_act(ndev - 1, p_b, h_b)
    fwd_out(ndev - 2, h_a)
    fwd_out(ndev - 1, h_b)

    small(3).wait()
    small(4).wait()
    for t in range(tasks):
        head = hts_in[t].astype(F32)
        hfs[8 * t:8 * t + ncls, dm * t:dm * (t + 1)] = head
    hcat[...] = hfs[...].astype(BF16)
    rows = hfs[:, 0:dm]
    for t in range(1, tasks):
        rows = rows + hfs[:, dm * t:dm * (t + 1)]
    hrow[...] = rows.astype(BF16)

    zs[...] = (xs[...].astype(F32) + zacc[...]).astype(BF16)
    logits = dot_nt(hrow[...], zs[...])
    cls = lax.broadcasted_iota(jnp.int32, (8, tok), 0)
    errs = []
    for t in range(tasks):
        lg = jnp.where(cls < ncls, logits[8 * t:8 * t + 8], -jnp.inf)
        e = jnp.exp(lg - jnp.max(lg, axis=0, keepdims=True))
        prob = e / jnp.sum(e, axis=0, keepdims=True)
        errs.append(prob - (cls == labs[t:t + 1, :]).astype(F32))
    errs.append(jnp.zeros((8, tok), F32))
    err_t = jnp.concatenate(errs, axis=0).T.astype(BF16)
    for t in range(tasks):
        dzs[t] = dot(err_t, hcat[:, dm * t:dm * (t + 1)]).astype(BF16)

    pl.semaphore_wait(barrier, ndev - 1)

    def blk(s):
        return lax.rem(me + 1 + s, ndev)

    def bwd_a(s, dp_ref):
        b = blk(s)
        for t in range(tasks):
            dp_ref[t] = (dot_nt(dzs[t], w2s[b]) * slope[b]).astype(BF16)

    def bwd_b(s, dp_ref):
        b = blk(s)
        bm = block_of(bms, b)
        for t in range(tasks):
            gbs[s, 8 * t:8 * t + 8] = dot(uts[...], dp_ref[t])
            dlacc[8 * t:8 * t + 8] += dot_nt(bm, dp_ref[t])

    def gb_send(s):
        return pltpu.make_async_remote_copy(src_ref=gbs.at[s], dst_ref=gbr.at[s], send_sem=gb_ss.at[s], recv_sem=gb_rs.at[s],
                                            device_id=(blk(s),), device_id_type=MESH)

    dps = (dp_a, dp_b)
    bwd_a(0, dp_a)

    def bwd_pair(i, carry):
        for k in range(2):
            s = 2 * i + k
            bwd_a(s + 1, dps[1 - k])
            bwd_b(s, dps[k])
            gb_send(s).start()
        return carry

    lax.fori_loop(0, (ndev - 2) // 2, bwd_pair, 0)
    bwd_a(ndev - 1, dp_b)
    bwd_b(ndev - 2, dp_a)
    gb_send(ndev - 2).start()
    bwd_b(ndev - 1, dp_b)

    ga_t = dot(dlacc[...].astype(BF16), xs[...])
    for k in range(ndev):
        gas[k] = ga_t[:8 * tasks, own * k:own * (k + 1)]

    def ga_send(off):
        peer = lax.rem(me + off, ndev)
        return pltpu.make_async_remote_copy(src_ref=gas.at[peer], dst_ref=gar.at[off - 1], send_sem=ga_ss.at[off - 1], recv_sem=ga_rs.at[off - 1],
                                            device_id=(peer,), device_id_type=MESH)

    for off in range(1, ndev):
        ga_send(off).start()

    gb_sum = gbs[ndev - 1]
    for s in range(ndev - 1):
        gb_send(s).wait_recv()
        gb_sum = gb_sum + gbr[s]
    gb_sum = gb_sum * (1.0 / batch_total)

    pairs = [(t, s) for t in range(tasks) for s in range(t, tasks)]
    gram_b = []
    for t, s in pairs:
        prod = gb_sum[8 * t:8 * t + 8] * gb_sum[8 * s:8 * s + 8]
        tot = prod[:, 0:128]
        for k in range(1, fb // 128):
            tot = tot + prod[:, 128 * k:128 * (k + 1)]
        gram_b.append(tot)

    ga_sum = gas[me]
    for off in range(1, ndev):
        ga_send(off).wait_recv()
        ga_sum = ga_sum + gar[off - 1]
    ga_sum = ga_sum * (1.0 / batch_total)

    ms[...] = jnp.zeros_like(ms)
    for p, (t, s) in enumerate(pairs):
        prod = ga_sum[8 * t:8 * t + 8] * ga_sum[8 * s:8 * s + 8] + gram_b[p]
        ms[p:p + 1, :] = jnp.sum(prod, axis=0, keepdims=True)

    def m_send(off):
        peer = lax.rem(me + off, ndev)
        return pltpu.make_async_remote_copy(src_ref=ms, dst_ref=mr.at[me], send_sem=m_ss.at[off - 1], recv_sem=m_rs.at[off - 1],
                                            device_id=(peer,), device_id_type=MESH)

    for off in range(1, ndev):
        m_send(off).start()
    mr[me] = ms[...]
    for off in range(1, ndev):
        m_send(off).wait_recv()
    m_tot = mr[0]
    for k in range(1, ndev):
        m_tot = m_tot + mr[k]
    m_tot = jnp.sum(m_tot, axis=1, keepdims=True)
    m_all = jnp.broadcast_to(m_tot, (8, 128))

    gram = {}
    for p, (t, s) in enumerate(pairs):
        gram[t, s] = gram[s, t] = jnp.broadcast_to(m_all[p:p + 1, :], (8, 128))
    trace = gram[0, 0]
    for t in range(1, tasks):
        trace = trace + gram[t, t]
    scale = trace / tasks
    gram = {key: val / scale for key, val in gram.items() if key[0] <= key[1]}

    def eg_step(_, wts):
        new = []
        for t in range(tasks):
            acc = gram[min(t, 0), max(t, 0)] * wts[0]
            for s in range(1, tasks):
                acc = acc + gram[min(t, s), max(t, s)] * wts[s]
            new.append(wts[t] * jnp.exp(-acc))
        tot = new[0]
        for t in range(1, tasks):
            tot = tot + new[t]
        inv = 1.0 / tot
        return tuple(w * inv for w in new)

    wts = lax.fori_loop(0, EG_STEPS, eg_step, tuple(jnp.full((8, 128), 1.0 / tasks, F32) for _ in range(tasks)))

    ga = wts[0] * ga_sum[0:8]
    for t in range(1, tasks):
        ga = ga + wts[t] * ga_sum[8 * t:8 * t + 8]
    ga_ref[...] = ga
    for k in range(fb // 128):
        cols = slice(128 * k, 128 * (k + 1))
        gb = wts[0] * gb_sum[0:8, cols]
        for t in range(1, tasks):
            gb = gb + wts[t] * gb_sum[8 * t:8 * t + 8, cols]
        gb_ref[:, cols] = gb
    lane = lax.broadcasted_iota(jnp.int32, (8, 128), 1)
    alpha = wts[tasks - 1]
    for t in range(tasks - 1):
        alpha = jnp.where(lane == t, wts[t], alpha)
    alpha_ref[...] = alpha[0:1, 0:tasks]

    for s in range(ndev - 1):
        gb_send(s).wait_send()
    for off in range(1, ndev):
        ga_send(off).wait_send()
        m_send(off).wait_send()


def solution(mesh):
    num_dev = mesh.shape["data"]

    def device_step(tokens, labels, w_one, w_two, adapter_a, adapter_b, task_heads):
        tok, dm = tokens.shape
        rank, dff = adapter_b.shape
        tasks, _, ncls = task_heads.shape
        fb = dff // num_dev
        own = dm // num_dev
        prow = 8 * tasks + 8
        dma = pltpu.SemaphoreType.DMA
        hbm = pl.BlockSpec(memory_space=pl.ANY)
        vmem = pl.BlockSpec(memory_space=pltpu.VMEM)
        alpha, ga, gb = pl.pallas_call(
            functools.partial(fused_kernel, num_dev, float(tok * num_dev)),
            name="fused_grads",
            out_shape=(jax.ShapeDtypeStruct((1, tasks), F32), jax.ShapeDtypeStruct((rank, own), F32), jax.ShapeDtypeStruct((rank, fb), F32)),
            in_specs=[hbm] * 7,
            out_specs=(vmem, vmem, vmem),
            scratch_shapes=[
                pltpu.VMEM((tok, dm), BF16),
                pltpu.VMEM((num_dev, dm, fb), BF16),
                pltpu.VMEM((num_dev, fb, dm), BF16),
                pltpu.VMEM((rank, dm), BF16),
                pltpu.VMEM((rank, dff), BF16),
                pltpu.VMEM((tasks, ncls, dm), BF16),
                pltpu.VMEM((tasks, tok), jnp.int32),
                pltpu.VMEM((rank, tok), BF16),
                pltpu.VMEM((tok, rank), BF16),
                pltpu.VMEM((tok, fb), F32),
                pltpu.VMEM((tok, fb), F32),
                pltpu.VMEM((tok, fb), BF16),
                pltpu.VMEM((tok, fb), BF16),
                pltpu.VMEM((num_dev, tok, fb), F32),
                pltpu.VMEM((tok, dm), F32),
                pltpu.VMEM((tok, dm), BF16),
                pltpu.VMEM((prow, tasks * dm), F32),
                pltpu.VMEM((prow, dm), BF16),
                pltpu.VMEM((prow, tasks * dm), BF16),
                pltpu.VMEM((tasks, tok, dm), BF16),
                pltpu.VMEM((tasks, tok, fb), BF16),
                pltpu.VMEM((tasks, tok, fb), BF16),
                pltpu.VMEM((prow, tok), F32),
                pltpu.VMEM((num_dev, 8 * tasks, fb), F32),
                pltpu.VMEM((num_dev - 1, 8 * tasks, fb), F32),
                pltpu.VMEM((num_dev, 8 * tasks, own), F32),
                pltpu.VMEM((num_dev - 1, 8 * tasks, own), F32),
                pltpu.VMEM((8, 128), F32),
                pltpu.VMEM((num_dev, 8, 128), F32),
                dma((num_dev,)),
                dma((num_dev,)),
                dma((5,)),
                dma((num_dev - 1,)),
                dma((num_dev - 1,)),
                dma((num_dev - 1,)),
                dma((num_dev - 1,)),
                dma((num_dev - 1,)),
                dma((num_dev - 1,)),
            ],
            compiler_params=pltpu.CompilerParams(collective_id=0, has_side_effects=True, vmem_limit_bytes=60 * 1024 * 1024),
        )(tokens, labels, w_one, w_two, adapter_a.T, adapter_b, jnp.transpose(task_heads, (0, 2, 1)))
        return alpha.reshape(tasks), ga.T, gb

    return jax.shard_map(device_step, mesh=mesh, in_specs=(P("data", None), P(None, "data"), P(), P(), P(), P(), P()), out_specs=(P(), P("data", None), P(None, "data")), check_vma=False)
```

```python
import functools

import jax
import jax.numpy as jnp
import numpy as np
from jax import lax
from jax.experimental import pallas as pl
from jax.experimental.pallas import tpu as pltpu
from jax.sharding import PartitionSpec as P

EG_STEPS = 20
MESH = pl.DeviceIdType.MESH
F32, BF16 = jnp.float32, jnp.bfloat16
GELU_C = float(np.sqrt(2.0 / np.pi))
GELU_A = 0.044715
NT = (((1,), (1,)), ((), ()))


def dot(lhs, rhs):
    return jnp.dot(lhs, rhs, preferred_element_type=F32)


def dot_nt(lhs, rhs):
    return lax.dot_general(lhs, rhs, NT, preferred_element_type=F32)


def fused_kernel(ndev, batch_total, x_hbm, lab_hbm, w1_hbm, w2_hbm, at_hbm, bm_hbm, ht_hbm,
                 m_out, ga_out, gb_out,
                 xs, w1s, w2s, ats, bms, hts_in, labs, uts, us, p_a, p_b, h_a, h_b, slope, zacc,
                 hfs, hrow, hcat, dzs, dp_a, dp_b, dlacc, gbs, gbr, gas, gar, ms, mr,
                 w1sem, w2sem, insem, gb_ss, gb_rs, ga_ss, ga_rs, m_ss, m_rs):
    tok = xs.shape[0]
    dff = w2_hbm.shape[0]
    fb = dff // ndev
    rank = ats.shape[0]
    tasks = hts_in.shape[0]
    ncls = hts_in.shape[1]
    dm = xs.shape[1]
    own = dm // ndev
    me = lax.axis_index("data")

    barrier = pltpu.get_barrier_semaphore()
    for off in range(1, ndev):
        pl.semaphore_signal(barrier, inc=1, device_id=(lax.rem(me + off, ndev),), device_id_type=MESH)

    def small(i):
        pairs = [(at_hbm, ats), (x_hbm, xs), (bm_hbm, bms), (ht_hbm, hts_in), (lab_hbm, labs)]
        return pltpu.make_async_copy(pairs[i][0], pairs[i][1], insem.at[i])

    def w1_copy(j):
        return pltpu.make_async_copy(w1_hbm.at[:, pl.ds(pl.multiple_of(j * fb, fb), fb)], w1s.at[j], w1sem.at[j])

    def w2_copy(j):
        return pltpu.make_async_copy(w2_hbm.at[pl.ds(pl.multiple_of(j * fb, fb), fb), :], w2s.at[j], w2sem.at[j])

    for i in (3, 0, 1):
        small(i).start()
    w1_copy(0).start()
    w1_copy(1).start()
    small(2).start()
    small(4).start()
    w2_copy(0).start()
    for j in range(2, ndev):
        w1_copy(j).start()
        w2_copy(j - 1).start()
    w2_copy(ndev - 1).start()

    zacc[...] = jnp.zeros_like(zacc)
    dlacc[...] = jnp.zeros_like(dlacc)
    hfs[...] = jnp.zeros_like(hfs)
    small(3).wait()
    for t in range(tasks):
        hfs[8 * t:8 * t + ncls, dm * t:dm * (t + 1)] = hts_in[t].astype(F32)
    hcat[...] = hfs[...].astype(BF16)
    head_rows = hfs[:, 0:dm]
    for t in range(1, tasks):
        head_rows = head_rows + hfs[:, dm * t:dm * (t + 1)]
    hrow[...] = head_rows.astype(BF16)

    small(0).wait()
    small(1).wait()
    ut = dot_nt(ats[...], xs[...])
    uts[...] = ut.astype(BF16)
    us[...] = ut.T.astype(BF16)
    small(2).wait()
    small(4).wait()
    w1_copy(0).wait()
    w1_copy(1).wait()

    def block_of(ref, j):
        return ref[:, pl.ds(pl.multiple_of(j * fb, fb), fb)]

    half, quarter = tok // 2, tok // 4

    def fwd_in(j, p_ref, i):
        rows = slice(half * i, half * (i + 1))
        p_ref[rows] = dot(xs[rows], w1s[j]) + dot(us[rows], block_of(bms, j))

    def fwd_act(j, p_ref, h_ref, i):
        rows = slice(quarter * i, quarter * (i + 1))
        x = p_ref[rows]
        x2 = x * x
        t = jnp.tanh(x * (GELU_C + (GELU_C * GELU_A) * x2))
        cdf = 0.5 + 0.5 * t
        h_ref[rows] = (x * cdf).astype(BF16)
        w = cdf * (1.0 - cdf)
        slope[j, rows] = cdf + x * (w * (2.0 * GELU_C + (6.0 * GELU_C * GELU_A) * x2))

    def fwd_out(j, h_ref, i):
        rows = slice(half * i, half * (i + 1))
        zacc[rows] += dot(h_ref[rows], w2s[j])

    ps, hs = (p_a, p_b), (h_a, h_b)
    for i in range(2):
        fwd_in(0, p_a, i)
    for i in range(2):
        fwd_in(1, p_b, i)
        fwd_act(0, p_a, h_a, 2 * i)
        fwd_act(0, p_a, h_a, 2 * i + 1)

    def fwd_pair(i, carry):
        for k in range(2):
            w1_copy(2 * i + k + 2).wait()
            w2_copy(2 * i + k).wait()
        for k in range(2):
            j = 2 * i + k
            for q in range(4):
                if q < 2:
                    fwd_in(j + 2, ps[k], q)
                else:
                    fwd_out(j, hs[k], q - 2)
                fwd_act(j + 1, ps[1 - k], hs[1 - k], q)
        return carry

    lax.fori_loop(0, (ndev - 2) // 2, fwd_pair, 0)
    w2_copy(ndev - 2).wait()
    w2_copy(ndev - 1).wait()
    for i in range(2):
        fwd_out(ndev - 2, h_a, i)
        fwd_act(ndev - 1, p_b, h_b, 2 * i)
        fwd_act(ndev - 1, p_b, h_b, 2 * i + 1)
    cls = lax.broadcasted_iota(jnp.int32, (8, half), 0)
    zs = []
    for i in range(2):
        rows = slice(half * i, half * (i + 1))
        zs.append((xs[rows].astype(F32) + (zacc[rows] + dot(h_b[rows], w2s[ndev - 1]))).astype(BF16))
    logits = [dot_nt(hrow[...], z) for z in zs]
    for i in range(2):
        rows = slice(half * i, half * (i + 1))
        errs = []
        for t in range(tasks):
            lg = jnp.where(cls < ncls, logits[i][8 * t:8 * t + 8], -jnp.inf)
            e = jnp.exp(lg - jnp.max(lg, axis=0, keepdims=True))
            prob = e / jnp.sum(e, axis=0, keepdims=True)
            errs.append(prob - (cls == labs[t:t + 1, rows]).astype(F32))
        errs.append(jnp.zeros((8, half), F32))
        err_t = jnp.concatenate(errs, axis=0).T.astype(BF16)
        for t in range(tasks):
            dzs[t, rows] = dot(err_t, hcat[:, dm * t:dm * (t + 1)]).astype(BF16)

    pl.semaphore_wait(barrier, ndev - 1)

    def blk(s):
        flip = ndev - 1 - s
        b, w = 0, 1
        while w < ndev:
            b = b + w * lax.rem(me // w + flip // w, 2)
            w *= 2
        return b

    def bwd_a(s, dp_ref):
        b = blk(s)
        for t in range(tasks):
            dp_ref[t] = (dot_nt(dzs[t], w2s[b]) * slope[b]).astype(BF16)

    def bwd_low(s, dp_ref):
        bm = block_of(bms, blk(s))
        for t in range(tasks):
            dlacc[8 * t:8 * t + 8] += dot_nt(bm, dp_ref[t])

    def bwd_col(s, dp_ref):
        for t in range(tasks):
            gbs[s, 8 * t:8 * t + 8] = dot(uts[...], dp_ref[t])

    def gb_send(s):
        return pltpu.make_async_remote_copy(src_ref=gbs.at[s], dst_ref=gbr.at[s], send_sem=gb_ss.at[s], recv_sem=gb_rs.at[s],
                                            device_id=(blk(s),), device_id_type=MESH)

    dps = (dp_a, dp_b)
    bwd_a(0, dp_a)

    def bwd_pair(i, carry):
        for k in range(2):
            s = 2 * i + k
            bwd_a(s + 1, dps[1 - k])
            bwd_low(s, dps[k])
            bwd_col(s, dps[k])
        for k in range(2):
            gb_send(2 * i + k).start()
        return carry

    lax.fori_loop(0, (ndev - 2) // 2, bwd_pair, 0)
    bwd_a(ndev - 1, dp_b)
    bwd_low(ndev - 2, dp_a)
    bwd_low(ndev - 1, dp_b)

    ga_t = dot(dlacc[...].astype(BF16), xs[...])
    for k in range(ndev):
        gas[k] = ga_t[:8 * tasks, own * k:own * (k + 1)]

    def ga_send(off):
        peer = lax.rem(me + off, ndev)
        return pltpu.make_async_remote_copy(src_ref=gas.at[peer], dst_ref=gar.at[off - 1], send_sem=ga_ss.at[off - 1], recv_sem=ga_rs.at[off - 1],
                                            device_id=(peer,), device_id_type=MESH)

    for off in range(1, ndev):
        ga_send(off).start()

    bwd_col(ndev - 2, dp_a)
    gb_send(ndev - 2).start()
    bwd_col(ndev - 1, dp_b)
    gb_sum = gbs[ndev - 1]
    for s in range(ndev - 1):
        gb_send(s).wait_recv()
        gb_sum = gb_sum + gbr[s]
    gb_sum = gb_sum * (1.0 / batch_total)
    gb_out[...] = gb_sum

    pairs = [(t, s) for t in range(tasks) for s in range(t, tasks)]
    gram_b = []
    for t, s in pairs:
        prod = gb_sum[8 * t:8 * t + 8] * gb_sum[8 * s:8 * s + 8]
        tot = prod[:, 0:128]
        for k in range(1, fb // 128):
            tot = tot + prod[:, 128 * k:128 * (k + 1)]
        gram_b.append(tot)

    ga_sum = gas[me]
    for off in range(1, ndev):
        ga_send(off).wait_recv()
        ga_sum = ga_sum + gar[off - 1]
    ga_sum = ga_sum * (1.0 / batch_total)
    ga_out[...] = ga_sum

    ms[...] = jnp.zeros_like(ms)
    for p, (t, s) in enumerate(pairs):
        prod = ga_sum[8 * t:8 * t + 8] * ga_sum[8 * s:8 * s + 8] + gram_b[p]
        ms[p:p + 1, :] = jnp.sum(prod, axis=0, keepdims=True)

    def m_send(off):
        peer = lax.rem(me + off, ndev)
        return pltpu.make_async_remote_copy(src_ref=ms, dst_ref=mr.at[me], send_sem=m_ss.at[off - 1], recv_sem=m_rs.at[off - 1],
                                            device_id=(peer,), device_id_type=MESH)

    for off in range(1, ndev):
        m_send(off).start()
    mr[me] = ms[...]
    for off in range(1, ndev):
        m_send(off).wait_recv()
    m_tot = mr[0]
    for k in range(1, ndev):
        m_tot = m_tot + mr[k]
    m_out[...] = m_tot

    for s in range(ndev - 1):
        gb_send(s).wait_send()
    for off in range(1, ndev):
        ga_send(off).wait_send()
        m_send(off).wait_send()


def solve_kernel(tasks, m_ref, ga_in, gb_in, alpha_ref, ga_ref, gb_ref):
    m_all = jnp.broadcast_to(jnp.sum(m_ref[...], axis=1, keepdims=True), (8, 128))
    pairs = [(t, s) for t in range(tasks) for s in range(t, tasks)]
    gram = {pair: jnp.broadcast_to(m_all[p:p + 1, :], (8, 128)) for p, pair in enumerate(pairs)}
    trace = gram[0, 0]
    for t in range(1, tasks):
        trace = trace + gram[t, t]
    scale = trace / tasks
    gram = {pair: val / scale for pair, val in gram.items()}

    def eg_step(_, wts):
        new = []
        for t in range(tasks):
            acc = gram[0, t] * wts[0]
            for s in range(1, tasks):
                acc = acc + gram[min(t, s), max(t, s)] * wts[s]
            new.append(wts[t] * jnp.exp(-acc))
        tot = new[0]
        for t in range(1, tasks):
            tot = tot + new[t]
        inv = 1.0 / tot
        return tuple(w * inv for w in new)

    wts = lax.fori_loop(0, EG_STEPS, eg_step, tuple(jnp.full((8, 128), 1.0 / tasks, F32) for _ in range(tasks)))

    ga = wts[0] * ga_in[0:8]
    for t in range(1, tasks):
        ga = ga + wts[t] * ga_in[8 * t:8 * t + 8]
    ga_ref[...] = ga
    for k in range(gb_ref.shape[1] // 128):
        cols = slice(128 * k, 128 * (k + 1))
        gb = wts[0] * gb_in[0:8, cols]
        for t in range(1, tasks):
            gb = gb + wts[t] * gb_in[8 * t:8 * t + 8, cols]
        gb_ref[:, cols] = gb
    lane = lax.broadcasted_iota(jnp.int32, (8, 128), 1)
    alpha = wts[tasks - 1]
    for t in range(tasks - 1):
        alpha = jnp.where(lane == t, wts[t], alpha)
    alpha_ref[...] = alpha[0:1, 0:tasks]


def solution(mesh):
    num_dev = mesh.shape["data"]

    def device_step(tokens, labels, w_one, w_two, adapter_a, adapter_b, task_heads):
        tok, dm = tokens.shape
        rank, dff = adapter_b.shape
        tasks, _, ncls = task_heads.shape
        fb = dff // num_dev
        own = dm // num_dev
        prow = 8 * tasks + 8
        dma = pltpu.SemaphoreType.DMA
        hbm = pl.BlockSpec(memory_space=pltpu.HBM)
        vmem = pl.BlockSpec(memory_space=pltpu.VMEM)
        sums = pl.pallas_call(
            functools.partial(fused_kernel, num_dev, float(tok * num_dev)),
            name="fused_grads",
            out_shape=(jax.ShapeDtypeStruct((8, 128), F32), jax.ShapeDtypeStruct((8 * tasks, own), F32), jax.ShapeDtypeStruct((8 * tasks, fb), F32)),
            in_specs=[hbm] * 7,
            out_specs=(vmem, vmem, vmem),
            scratch_shapes=[
                pltpu.VMEM((tok, dm), BF16),
                pltpu.VMEM((num_dev, dm, fb), BF16),
                pltpu.VMEM((num_dev, fb, dm), BF16),
                pltpu.VMEM((rank, dm), BF16),
                pltpu.VMEM((rank, dff), BF16),
                pltpu.VMEM((tasks, ncls, dm), BF16),
                pltpu.VMEM((tasks, tok), jnp.int32),
                pltpu.VMEM((rank, tok), BF16),
                pltpu.VMEM((tok, rank), BF16),
                pltpu.VMEM((tok, fb), F32),
                pltpu.VMEM((tok, fb), F32),
                pltpu.VMEM((tok, fb), BF16),
                pltpu.VMEM((tok, fb), BF16),
                pltpu.VMEM((num_dev, tok, fb), F32),
                pltpu.VMEM((tok, dm), F32),
                pltpu.VMEM((prow, tasks * dm), F32),
                pltpu.VMEM((prow, dm), BF16),
                pltpu.VMEM((prow, tasks * dm), BF16),
                pltpu.VMEM((tasks, tok, dm), BF16),
                pltpu.VMEM((tasks, tok, fb), BF16),
                pltpu.VMEM((tasks, tok, fb), BF16),
                pltpu.VMEM((prow, tok), F32),
                pltpu.VMEM((num_dev, 8 * tasks, fb), F32),
                pltpu.VMEM((num_dev - 1, 8 * tasks, fb), F32),
                pltpu.VMEM((num_dev, 8 * tasks, own), F32),
                pltpu.VMEM((num_dev - 1, 8 * tasks, own), F32),
                pltpu.VMEM((8, 128), F32),
                pltpu.VMEM((num_dev, 8, 128), F32),
                dma((num_dev,)),
                dma((num_dev,)),
                dma((5,)),
                dma((num_dev - 1,)),
                dma((num_dev - 1,)),
                dma((num_dev - 1,)),
                dma((num_dev - 1,)),
                dma((num_dev - 1,)),
                dma((num_dev - 1,)),
            ],
            compiler_params=pltpu.CompilerParams(collective_id=0, has_side_effects=True, vmem_limit_bytes=48 * 1024 * 1024),
        )(*[pltpu.with_memory_space_constraint(arr, pltpu.HBM) for arr in (tokens, labels, w_one, w_two, adapter_a.T, adapter_b, jnp.transpose(task_heads, (0, 2, 1)))])
        alpha, ga, gb = pl.pallas_call(
            functools.partial(solve_kernel, tasks),
            name="solve",
            out_shape=(jax.ShapeDtypeStruct((1, tasks), F32), jax.ShapeDtypeStruct((rank, own), F32), jax.ShapeDtypeStruct((rank, fb), F32)),
            in_specs=[vmem] * 3,
            out_specs=(vmem,) * 3,
            compiler_params=pltpu.CompilerParams(vmem_limit_bytes=2 * 1024 * 1024),
        )(*sums)
        return alpha.reshape(tasks), ga.T, gb

    return jax.shard_map(device_step, mesh=mesh, in_specs=(P("data", None), P(None, "data"), P(), P(), P(), P(), P()), out_specs=(P(), P("data", None), P(None, "data")), check_vma=False)
```

```python
import functools

import jax
import jax.numpy as jnp
import numpy as np
from jax import lax
from jax.experimental import pallas as pl
from jax.experimental.pallas import tpu as pltpu
from jax.sharding import PartitionSpec as P

EG_STEPS = 20
MESH = pl.DeviceIdType.MESH
F32, BF16 = jnp.float32, jnp.bfloat16
GELU_C = float(np.sqrt(2.0 / np.pi))
GELU_A = 0.044715
NT = (((1,), (1,)), ((), ()))


def dot(lhs, rhs):
    return jnp.dot(lhs, rhs, preferred_element_type=F32)


def dot_nt(lhs, rhs):
    return lax.dot_general(lhs, rhs, NT, preferred_element_type=F32)


def fused_kernel(ndev, batch_total, x_hbm, lab_hbm, w1_hbm, w2_hbm, at_hbm, bm_hbm, ht_hbm,
                 m_out, ga_out, gb_out,
                 xs, w1s, w2s, ats, bms, hts_in, labs, uts, us, p_a, p_b, h_a, h_b, slope, zacc,
                 hrow, hcol, dzs, dp_a, dp_b, dlacc, gbs, gbr, gas, gar, ms, mr,
                 w1sem, w2sem, insem, gb_ss, gb_rs, ga_ss, ga_rs, m_ss, m_rs):
    tok = xs.shape[0]
    dff = w2_hbm.shape[0]
    fb = dff // ndev
    rank = ats.shape[0]
    tasks = hts_in.shape[0]
    ncls = hts_in.shape[1]
    dm = xs.shape[1]
    own = dm // ndev
    me = lax.axis_index("data")

    def peer_of(flip):
        b, w = 0, 1
        while w < ndev:
            b = b + w * lax.rem(me // w + flip // w, 2)
            w *= 2
        return b

    far_first = range(ndev - 1, 0, -1)

    def small(i):
        pairs = [(at_hbm, ats), (x_hbm, xs), (bm_hbm, bms), (ht_hbm, hts_in), (lab_hbm, labs)]
        return pltpu.make_async_copy(pairs[i][0], pairs[i][1], insem.at[i])

    def w1_copy(j):
        return pltpu.make_async_copy(w1_hbm.at[:, pl.ds(pl.multiple_of(j * fb, fb), fb)], w1s.at[j], w1sem.at[j])

    def w2_copy(j):
        return pltpu.make_async_copy(w2_hbm.at[pl.ds(pl.multiple_of(j * fb, fb), fb), :], w2s.at[j], w2sem.at[j])

    for i in (1, 0, 3):
        small(i).start()
    w1_copy(0).start()
    w1_copy(1).start()
    small(2).start()
    small(4).start()
    w2_copy(0).start()
    for j in range(2, ndev):
        w1_copy(j).start()
        w2_copy(j - 1).start()
    w2_copy(ndev - 1).start()

    barrier = pltpu.get_barrier_semaphore()
    for flip in far_first:
        pl.semaphore_signal(barrier, inc=1, device_id=(peer_of(flip),), device_id_type=MESH)

    zacc[...] = jnp.zeros_like(zacc)
    dlacc[...] = jnp.zeros_like(dlacc)
    small(3).wait()
    pad = jnp.zeros((8 - ncls, dm), F32)
    heads = []
    for t in range(tasks):
        heads += [hts_in[t].astype(F32), pad]
    heads = jnp.concatenate(heads + [jnp.zeros((8, dm), F32)], axis=0)
    hrow[...] = heads.astype(BF16)
    hcol[...] = heads.T.astype(BF16)

    small(0).wait()
    small(1).wait()
    ut = dot_nt(ats[...], xs[...])
    uts[...] = ut.astype(BF16)
    us[...] = ut.T.astype(BF16)
    small(2).wait()
    small(4).wait()
    w1_copy(0).wait()
    w1_copy(1).wait()

    def block_of(ref, j):
        return ref[:, pl.ds(pl.multiple_of(j * fb, fb), fb)]

    half, quarter = tok // 2, tok // 4

    def fwd_in(j, p_ref, i):
        rows = slice(half * i, half * (i + 1))
        p_ref[rows] = dot(xs[rows], w1s[j]) + dot(us[rows], block_of(bms, j))

    def fwd_act(j, p_ref, h_ref, i):
        rows = slice(quarter * i, quarter * (i + 1))
        x = p_ref[rows]
        x2 = x * x
        t = jnp.tanh(x * (GELU_C + (GELU_C * GELU_A) * x2))
        cdf = 0.5 + 0.5 * t
        h_ref[rows] = (x * cdf).astype(BF16)
        w = cdf * (1.0 - cdf)
        slope[j, :, rows] = (cdf + x * (w * (2.0 * GELU_C + (6.0 * GELU_C * GELU_A) * x2))).T

    def fwd_out(j, h_ref):
        zacc[...] += dot(h_ref[...], w2s[j])

    ps, hs = (p_a, p_b), (h_a, h_b)
    for i in range(2):
        fwd_in(0, p_a, i)
    for i in range(2):
        fwd_in(1, p_b, i)
        fwd_act(0, p_a, h_a, 2 * i)
        fwd_act(0, p_a, h_a, 2 * i + 1)

    def fwd_pair(i, carry):
        for k in range(2):
            w1_copy(2 * i + k + 2).wait()
            w2_copy(2 * i + k).wait()
        for k in range(2):
            j = 2 * i + k
            for q in range(4):
                if q < 2:
                    fwd_in(j + 2, ps[k], q)
                elif q == 2:
                    fwd_out(j, hs[k])
                fwd_act(j + 1, ps[1 - k], hs[1 - k], q)
        return carry

    lax.fori_loop(0, (ndev - 2) // 2, fwd_pair, 0)
    pl.semaphore_wait(barrier, ndev - 1)
    w2_copy(ndev - 2).wait()
    w2_copy(ndev - 1).wait()
    fwd_out(ndev - 2, h_a)
    for i in range(2):
        fwd_act(ndev - 1, p_b, h_b, 2 * i)
        fwd_act(ndev - 1, p_b, h_b, 2 * i + 1)
    cls = lax.broadcasted_iota(jnp.int32, (8, half), 0)
    z = (xs[...].astype(F32) + (zacc[...] + dot(h_b[...], w2s[ndev - 1]))).astype(BF16)
    both = dot_nt(hrow[...], z)
    logits = [both[:, :half], both[:, half:]]
    errs = [[] for _ in range(tasks)]
    for i in range(2):
        rows = slice(half * i, half * (i + 1))
        for t in range(tasks):
            lg = jnp.where(cls < ncls, logits[i][8 * t:8 * t + 8], -jnp.inf)
            e = jnp.exp(lg - jnp.max(lg, axis=0, keepdims=True))
            prob = e / jnp.sum(e, axis=0, keepdims=True)
            errs[t].append(prob - (cls == labs[t:t + 1, rows]).astype(F32))
    blank = jnp.zeros((8, tok), F32)
    for t in range(tasks):
        err = jnp.concatenate([jnp.concatenate(errs[t], axis=1) if k == t else blank for k in range(tasks + 1)], axis=0)
        dzs[t] = dot(hcol[...], err.astype(BF16)).astype(BF16)


    def blk(s):
        return peer_of(ndev - 1 - s)

    def low_piece(s, dp_ref, t, i):
        part = slice(fb // 2 * i, fb // 2 * (i + 1))
        return dot(block_of(bms, blk(s))[:, part], dp_ref[t, part, :])

    def col_piece(dp_ref, t, i):
        part = slice(tok // 2 * i, tok // 2 * (i + 1))
        return dot_nt(uts[:, part], dp_ref[t, :, part])

    def bwd_step(s, dp_new, dp_old, cols=True):
        b = blk(s)
        for t in range(tasks):
            dh, low, col = None, [], []
            for q in range(4):
                part = slice(dm // 4 * q, dm // 4 * (q + 1))
                piece = dot(w2s[b, :, part], dzs[t, part, :])
                dh = piece if dh is None else dh + piece
                if dp_old is not None:
                    if q % 2 == 0 and cols:
                        col.append(col_piece(dp_old, t, q // 2))
                    if q % 2 == 1:
                        low.append(low_piece(s - 1, dp_old, t, q // 2))
            dp_new[t] = (dh * slope[b]).astype(BF16)
            if low:
                dlacc[8 * t:8 * t + 8] += low[0] + low[1]
            if col:
                gbs[s - 1, 8 * t:8 * t + 8] = col[0] + col[1]

    def bwd_low(s, dp_ref):
        for t in range(tasks):
            dlacc[8 * t:8 * t + 8] += low_piece(s, dp_ref, t, 0) + low_piece(s, dp_ref, t, 1)

    def bwd_col(s, dp_ref):
        for t in range(tasks):
            gbs[s, 8 * t:8 * t + 8] = col_piece(dp_ref, t, 0) + col_piece(dp_ref, t, 1)

    def gb_send(s):
        return pltpu.make_async_remote_copy(src_ref=gbs.at[s], dst_ref=gbr.at[s], send_sem=gb_ss.at[s], recv_sem=gb_rs.at[s],
                                            device_id=(blk(s),), device_id_type=MESH)

    dps = (dp_a, dp_b)
    bwd_step(0, dp_a, None)

    def bwd_pair(i, carry):
        for k in range(2):
            bwd_step(2 * i + k + 1, dps[1 - k], dps[k])
        for k in range(2):
            gb_send(2 * i + k).start()
        return carry

    lax.fori_loop(0, (ndev - 2) // 2, bwd_pair, 0)
    bwd_step(ndev - 1, dp_b, dp_a, cols=False)
    bwd_low(ndev - 1, dp_b)

    ga_t = dot(dlacc[...].astype(BF16), xs[...])
    for k in range(ndev):
        gas[k] = ga_t[:8 * tasks, own * k:own * (k + 1)]

    def ga_send(off):
        peer = peer_of(off)
        return pltpu.make_async_remote_copy(src_ref=gas.at[peer], dst_ref=gar.at[off - 1], send_sem=ga_ss.at[off - 1], recv_sem=ga_rs.at[off - 1],
                                            device_id=(peer,), device_id_type=MESH)

    for off in far_first:
        ga_send(off).start()

    bwd_col(ndev - 2, dp_a)
    gb_send(ndev - 2).start()
    bwd_col(ndev - 1, dp_b)
    gb_sum = gbs[ndev - 1]
    for s in range(ndev - 1):
        gb_send(s).wait_recv()
        gb_sum = gb_sum + gbr[s]
    gb_sum = gb_sum * (1.0 / batch_total)
    gb_out[...] = gb_sum

    pairs = [(t, s) for t in range(tasks) for s in range(t, tasks)]
    gram_b = []
    for t, s in pairs:
        prod = gb_sum[8 * t:8 * t + 8] * gb_sum[8 * s:8 * s + 8]
        tot = prod[:, 0:128]
        for k in range(1, fb // 128):
            tot = tot + prod[:, 128 * k:128 * (k + 1)]
        gram_b.append(tot)

    ga_sum = gas[me]
    for off in range(1, ndev):
        ga_send(off).wait_recv()
        ga_sum = ga_sum + gar[off - 1]
    ga_sum = ga_sum * (1.0 / batch_total)
    ga_out[...] = ga_sum

    rows = []
    for p, (t, s) in enumerate(pairs):
        prod = ga_sum[8 * t:8 * t + 8] * ga_sum[8 * s:8 * s + 8] + gram_b[p]
        rows.append(jnp.sum(prod, axis=0, keepdims=True))
    lane = lax.broadcasted_iota(jnp.int32, (1, 128), 1)
    m_own = jnp.zeros((1, 128), F32)
    for p, row in enumerate(rows):
        m_own = jnp.where(lane == p, jnp.sum(row, axis=1, keepdims=True), m_own)
    ms[...] = m_own

    def m_send(off):
        peer = peer_of(off)
        return pltpu.make_async_remote_copy(src_ref=ms, dst_ref=mr.at[me], send_sem=m_ss.at[off - 1], recv_sem=m_rs.at[off - 1],
                                            device_id=(peer,), device_id_type=MESH)

    for off in far_first:
        m_send(off).start()
    mr[me] = ms[...]
    for off in range(1, ndev):
        m_send(off).wait_recv()
    m_tot = mr[0]
    for k in range(1, ndev):
        m_tot = m_tot + mr[k]
    m_out[...] = m_tot

    for s in range(ndev - 1):
        gb_send(s).wait_send()
    for off in range(1, ndev):
        ga_send(off).wait_send()
        m_send(off).wait_send()


def solve_kernel(tasks, m_ref, ga_in, gb_in, alpha_ref, ga_ref, gb_ref):
    m_all = m_ref[...]
    pairs = [(t, s) for t in range(tasks) for s in range(t, tasks)]
    gram = {pair: jnp.broadcast_to(m_all[:, p:p + 1], (8, 128)) for p, pair in enumerate(pairs)}
    trace = gram[0, 0]
    for t in range(1, tasks):
        trace = trace + gram[t, t]
    scale = trace / tasks
    gram = {pair: val / scale for pair, val in gram.items()}

    def eg_step(_, wts):
        new = []
        for t in range(tasks):
            acc = gram[0, t] * wts[0]
            for s in range(1, tasks):
                acc = acc + gram[min(t, s), max(t, s)] * wts[s]
            new.append(wts[t] * jnp.exp(-acc))
        tot = new[0]
        for t in range(1, tasks):
            tot = tot + new[t]
        inv = 1.0 / tot
        return tuple(w * inv for w in new)

    wts = lax.fori_loop(0, EG_STEPS, eg_step, tuple(jnp.full((8, 128), 1.0 / tasks, F32) for _ in range(tasks)), unroll=5)

    ga = wts[0] * ga_in[0:8]
    for t in range(1, tasks):
        ga = ga + wts[t] * ga_in[8 * t:8 * t + 8]
    ga_ref[...] = ga
    for k in range(gb_ref.shape[1] // 128):
        cols = slice(128 * k, 128 * (k + 1))
        gb = wts[0] * gb_in[0:8, cols]
        for t in range(1, tasks):
            gb = gb + wts[t] * gb_in[8 * t:8 * t + 8, cols]
        gb_ref[:, cols] = gb
    lane = lax.broadcasted_iota(jnp.int32, (8, 128), 1)
    alpha = wts[tasks - 1]
    for t in range(tasks - 1):
        alpha = jnp.where(lane == t, wts[t], alpha)
    alpha_ref[...] = alpha[0:1, 0:tasks]


def solution(mesh):
    num_dev = mesh.shape["data"]

    def device_step(tokens, labels, w_one, w_two, adapter_a, adapter_b, task_heads):
        tok, dm = tokens.shape
        rank, dff = adapter_b.shape
        tasks, _, ncls = task_heads.shape
        fb = dff // num_dev
        own = dm // num_dev
        prow = 8 * tasks + 8
        dma = pltpu.SemaphoreType.DMA
        hbm = pl.BlockSpec(memory_space=pltpu.HBM)
        vmem = pl.BlockSpec(memory_space=pltpu.VMEM)
        sums = pl.pallas_call(
            functools.partial(fused_kernel, num_dev, float(tok * num_dev)),
            name="fused_grads",
            out_shape=(jax.ShapeDtypeStruct((1, 128), F32), jax.ShapeDtypeStruct((8 * tasks, own), F32), jax.ShapeDtypeStruct((8 * tasks, fb), F32)),
            in_specs=[hbm] * 7,
            out_specs=(vmem, vmem, vmem),
            scratch_shapes=[
                pltpu.VMEM((tok, dm), BF16),
                pltpu.VMEM((num_dev, dm, fb), BF16),
                pltpu.VMEM((num_dev, fb, dm), BF16),
                pltpu.VMEM((rank, dm), BF16),
                pltpu.VMEM((rank, dff), BF16),
                pltpu.VMEM((tasks, ncls, dm), BF16),
                pltpu.VMEM((tasks, tok), jnp.int32),
                pltpu.VMEM((rank, tok), BF16),
                pltpu.VMEM((tok, rank), BF16),
                pltpu.VMEM((tok, fb), F32),
                pltpu.VMEM((tok, fb), F32),
                pltpu.VMEM((tok, fb), BF16),
                pltpu.VMEM((tok, fb), BF16),
                pltpu.VMEM((num_dev, fb, tok), F32),
                pltpu.VMEM((tok, dm), F32),
                pltpu.VMEM((prow, dm), BF16),
                pltpu.VMEM((dm, prow), BF16),
                pltpu.VMEM((tasks, dm, tok), BF16),
                pltpu.VMEM((tasks, fb, tok), BF16),
                pltpu.VMEM((tasks, fb, tok), BF16),
                pltpu.VMEM((prow, tok), F32),
                pltpu.VMEM((num_dev, 8 * tasks, fb), F32),
                pltpu.VMEM((num_dev - 1, 8 * tasks, fb), F32),
                pltpu.VMEM((num_dev, 8 * tasks, own), F32),
                pltpu.VMEM((num_dev - 1, 8 * tasks, own), F32),
                pltpu.VMEM((1, 128), F32),
                pltpu.VMEM((num_dev, 1, 128), F32),
                dma((num_dev,)),
                dma((num_dev,)),
                dma((5,)),
                dma((num_dev - 1,)),
                dma((num_dev - 1,)),
                dma((num_dev - 1,)),
                dma((num_dev - 1,)),
                dma((num_dev - 1,)),
                dma((num_dev - 1,)),
            ],
            compiler_params=pltpu.CompilerParams(collective_id=0, has_side_effects=True, vmem_limit_bytes=48 * 1024 * 1024),
        )(*[pltpu.with_memory_space_constraint(arr, pltpu.HBM) for arr in (tokens, labels, w_one, w_two, adapter_a.T, adapter_b, jnp.transpose(task_heads, (0, 2, 1)))])
        alpha, ga, gb = pl.pallas_call(
            functools.partial(solve_kernel, tasks),
            name="solve",
            out_shape=(jax.ShapeDtypeStruct((1, tasks), F32), jax.ShapeDtypeStruct((rank, own), F32), jax.ShapeDtypeStruct((rank, fb), F32)),
            in_specs=[vmem] * 3,
            out_specs=(vmem,) * 3,
            compiler_params=pltpu.CompilerParams(vmem_limit_bytes=2 * 1024 * 1024),
        )(*sums)
        return alpha.reshape(tasks), ga.T, gb

    return jax.shard_map(device_step, mesh=mesh, in_specs=(P("data", None), P(None, "data"), P(), P(), P(), P(), P()), out_specs=(P(), P("data", None), P(None, "data")), check_vma=False)
```

```python
import functools

import jax
import jax.numpy as jnp
import numpy as np
from jax import lax
from jax.experimental import pallas as pl
from jax.experimental.pallas import tpu as pltpu
from jax.sharding import PartitionSpec as P

EG_STEPS = 20
MESH = pl.DeviceIdType.MESH
F32, BF16 = jnp.float32, jnp.bfloat16
GELU_C = float(np.sqrt(2.0 / np.pi))
GELU_A = 0.044715
NT = (((1,), (1,)), ((), ()))


def dot(lhs, rhs):
    return jnp.dot(lhs, rhs, preferred_element_type=F32)


def dot_nt(lhs, rhs):
    return lax.dot_general(lhs, rhs, NT, preferred_element_type=F32)


def fused_kernel(ndev, batch_total, x_hbm, lab_hbm, w1_hbm, w2_hbm, at_hbm, bm_hbm, ht_hbm,
                 m_out, ga_out, gb_out,
                 xs, w1s, w2s, ats, bms, hts_in, labs, uts, us, p_a, p_b, h_a, h_b, h_c, slope, zacc,
                 hrow, hcol, dzs, dp_a, dp_b, dlacc, gbs, gbr, gas, gar, ms, mr,
                 w1sem, w2sem, insem, gb_ss, gb_rs, ga_ss, ga_rs, m_ss, m_rs):
    tok = xs.shape[0]
    dff = w2_hbm.shape[0]
    fb = dff // ndev
    rank = ats.shape[0]
    tasks = hts_in.shape[0]
    ncls = hts_in.shape[1]
    dm = xs.shape[1]
    own = dm // ndev
    me = lax.axis_index("data")

    def peer_of(flip):
        b, w = 0, 1
        while w < ndev:
            b = b + w * lax.rem(me // w + flip // w, 2)
            w *= 2
        return b

    far_first = range(ndev - 1, 0, -1)

    def small(i):
        pairs = [(at_hbm, ats), (x_hbm, xs), (bm_hbm, bms), (ht_hbm, hts_in), (lab_hbm, labs)]
        return pltpu.make_async_copy(pairs[i][0], pairs[i][1], insem.at[i])

    def w1_copy(j):
        return pltpu.make_async_copy(w1_hbm.at[:, pl.ds(pl.multiple_of(j * fb, fb), fb)], w1s.at[j], w1sem.at[j])

    def w2_copy(j):
        return pltpu.make_async_copy(w2_hbm.at[pl.ds(pl.multiple_of(j * fb, fb), fb), :], w2s.at[j], w2sem.at[j])

    for i in (1, 0, 3):
        small(i).start()
    w1_copy(0).start()
    w1_copy(1).start()
    small(2).start()
    small(4).start()
    w2_copy(0).start()
    for j in range(2, ndev):
        w1_copy(j).start()
        w2_copy(j - 1).start()
    w2_copy(ndev - 1).start()

    barrier = pltpu.get_barrier_semaphore()
    for flip in far_first:
        pl.semaphore_signal(barrier, inc=1, device_id=(peer_of(flip),), device_id_type=MESH)

    zacc[...] = jnp.zeros_like(zacc)
    dlacc[...] = jnp.zeros_like(dlacc)
    small(3).wait()
    pad = jnp.zeros((8 - ncls, dm), F32)
    heads = []
    for t in range(tasks):
        heads += [hts_in[t].astype(F32), pad]
    heads = jnp.concatenate(heads + [jnp.zeros((8, dm), F32)], axis=0)
    hrow[...] = heads.astype(BF16)
    hcol[...] = heads.T.astype(BF16)

    small(0).wait()
    small(1).wait()
    ut = dot_nt(ats[...], xs[...])
    uts[...] = ut.astype(BF16)
    us[...] = ut.T.astype(BF16)
    small(2).wait()
    small(4).wait()
    w1_copy(0).wait()
    w1_copy(1).wait()

    def block_of(ref, j):
        return ref[:, pl.ds(pl.multiple_of(j * fb, fb), fb)]

    half, quarter = tok // 2, tok // 4

    def fwd_in(j, p_ref, i):
        rows = slice(half * i, half * (i + 1))
        p_ref[rows] = dot(xs[rows], w1s[j]) + dot(us[rows], block_of(bms, j))

    def fwd_act(j, p_ref, h_ref, i):
        rows = slice(quarter * i, quarter * (i + 1))
        x = p_ref[rows]
        x2 = x * x
        t = jnp.tanh(x * (GELU_C + (GELU_C * GELU_A) * x2))
        cdf = 0.5 + 0.5 * t
        h_ref[rows] = (x * cdf).astype(BF16)
        w = cdf * (1.0 - cdf)
        slope[j, :, rows] = (cdf + x * (w * (2.0 * GELU_C + (6.0 * GELU_C * GELU_A) * x2))).T

    def fwd_out(j, h_ref):
        zacc[...] += dot(h_ref[...], w2s[j])

    ps, hs = (p_a, p_b), (h_a, h_b, h_c)
    for i in range(2):
        fwd_in(0, p_a, i)
    for i in range(2):
        fwd_in(1, p_b, i)
        fwd_act(0, p_a, h_a, 2 * i)
        fwd_act(0, p_a, h_a, 2 * i + 1)

    def fwd_pair(i, carry):
        for k in range(2):
            w1_copy(2 * i + k + 2).wait()
            w2_copy(2 * i + k).wait()
        for k in range(2):
            j = 2 * i + k
            for q in range(4):
                if q < 2:
                    fwd_in(j + 2, ps[k], q)
                fwd_act(j + 1, ps[1 - k], hs[1 + k], q)
        zacc[...] += dot(h_a[...], w2s[2 * i]) + dot(h_b[...], w2s[2 * i + 1])
        h_a[...] = h_c[...]
        return carry

    lax.fori_loop(0, (ndev - 2) // 2, fwd_pair, 0)
    pl.semaphore_wait(barrier, ndev - 1)
    w2_copy(ndev - 2).wait()
    w2_copy(ndev - 1).wait()
    fwd_out(ndev - 2, h_a)
    for i in range(2):
        fwd_act(ndev - 1, p_b, h_b, 2 * i)
        fwd_act(ndev - 1, p_b, h_b, 2 * i + 1)
    cls = lax.broadcasted_iota(jnp.int32, (8, half), 0)
    z = (xs[...].astype(F32) + (zacc[...] + dot(h_b[...], w2s[ndev - 1]))).astype(BF16)
    both = dot_nt(hrow[...], z)
    logits = [both[:, :half], both[:, half:]]
    errs = [[] for _ in range(tasks)]
    for i in range(2):
        rows = slice(half * i, half * (i + 1))
        for t in range(tasks):
            lg = jnp.where(cls < ncls, logits[i][8 * t:8 * t + 8], -jnp.inf)
            e = jnp.exp(lg - jnp.max(lg, axis=0, keepdims=True))
            prob = e / jnp.sum(e, axis=0, keepdims=True)
            errs[t].append(prob - (cls == labs[t:t + 1, rows]).astype(F32))
    blank = jnp.zeros((8, tok), F32)
    for t in range(tasks):
        err = jnp.concatenate([jnp.concatenate(errs[t], axis=1) if k == t else blank for k in range(tasks + 1)], axis=0)
        dzs[t] = dot(hcol[...], err.astype(BF16)).astype(BF16)


    def blk(s):
        return peer_of(ndev - 1 - s)

    def low_piece(s, dp_ref, t, i):
        part = slice(fb // 2 * i, fb // 2 * (i + 1))
        return dot(block_of(bms, blk(s))[:, part], dp_ref[t, part, :])

    def col_piece(dp_ref, t, i):
        part = slice(tok // 2 * i, tok // 2 * (i + 1))
        return dot_nt(uts[:, part], dp_ref[t, :, part])

    def bwd_step(s, dp_new, dp_old, cols=True):
        b = blk(s)
        for t in range(tasks):
            dh, low, col = None, [], []
            for q in range(4):
                part = slice(dm // 4 * q, dm // 4 * (q + 1))
                piece = dot(w2s[b, :, part], dzs[t, part, :])
                dh = piece if dh is None else dh + piece
                if dp_old is not None and q % 2 == 0:
                    if cols:
                        col.append(col_piece(dp_old, t, q // 2))
                    low.append(low_piece(s - 1, dp_old, t, q // 2))
            dp_new[t] = (dh * slope[b]).astype(BF16)
            if low:
                dlacc[8 * t:8 * t + 8] += low[0] + low[1]
            if col:
                gbs[s - 1, 8 * t:8 * t + 8] = col[0] + col[1]

    def bwd_low(s, dp_ref):
        for t in range(tasks):
            dlacc[8 * t:8 * t + 8] += low_piece(s, dp_ref, t, 0) + low_piece(s, dp_ref, t, 1)

    def bwd_col(s, dp_ref):
        for t in range(tasks):
            gbs[s, 8 * t:8 * t + 8] = col_piece(dp_ref, t, 0) + col_piece(dp_ref, t, 1)

    def gb_send(s):
        return pltpu.make_async_remote_copy(src_ref=gbs.at[s], dst_ref=gbr.at[s], send_sem=gb_ss.at[s], recv_sem=gb_rs.at[s],
                                            device_id=(blk(s),), device_id_type=MESH)

    dps = (dp_a, dp_b)
    bwd_step(0, dp_a, None)

    def bwd_pair(i, carry):
        for k in range(2):
            bwd_step(2 * i + k + 1, dps[1 - k], dps[k])
        for k in range(2):
            gb_send(2 * i + k).start()
        return carry

    lax.fori_loop(0, (ndev - 2) // 2, bwd_pair, 0)
    bwd_step(ndev - 1, dp_b, dp_a, cols=False)
    bwd_low(ndev - 1, dp_b)

    ga_t = dot(dlacc[...].astype(BF16), xs[...])
    for k in range(ndev):
        gas[k] = ga_t[:8 * tasks, own * k:own * (k + 1)]

    def ga_send(off):
        peer = peer_of(off)
        return pltpu.make_async_remote_copy(src_ref=gas.at[peer], dst_ref=gar.at[off - 1], send_sem=ga_ss.at[off - 1], recv_sem=ga_rs.at[off - 1],
                                            device_id=(peer,), device_id_type=MESH)

    for off in far_first:
        ga_send(off).start()

    bwd_col(ndev - 2, dp_a)
    gb_send(ndev - 2).start()
    bwd_col(ndev - 1, dp_b)
    gb_sum = gbs[ndev - 1]
    for s in range(ndev - 1):
        gb_send(s).wait_recv()
        gb_sum = gb_sum + gbr[s]
    gb_sum = gb_sum * (1.0 / batch_total)
    gb_out[...] = gb_sum

    pairs = [(t, s) for t in range(tasks) for s in range(t, tasks)]
    gram_b = []
    for t, s in pairs:
        prod = gb_sum[8 * t:8 * t + 8] * gb_sum[8 * s:8 * s + 8]
        tot = prod[:, 0:128]
        for k in range(1, fb // 128):
            tot = tot + prod[:, 128 * k:128 * (k + 1)]
        gram_b.append(tot)

    ga_sum = gas[me]
    for off in range(1, ndev):
        ga_send(off).wait_recv()
        ga_sum = ga_sum + gar[off - 1]
    ga_sum = ga_sum * (1.0 / batch_total)
    ga_out[...] = ga_sum

    rows = []
    for p, (t, s) in enumerate(pairs):
        prod = ga_sum[8 * t:8 * t + 8] * ga_sum[8 * s:8 * s + 8] + gram_b[p]
        rows.append(jnp.sum(prod, axis=0, keepdims=True))
    lane = lax.broadcasted_iota(jnp.int32, (1, 128), 1)
    m_own = jnp.zeros((1, 128), F32)
    for p, row in enumerate(rows):
        m_own = jnp.where(lane == p, jnp.sum(row, axis=1, keepdims=True), m_own)
    ms[...] = m_own

    def m_send(off):
        peer = peer_of(off)
        return pltpu.make_async_remote_copy(src_ref=ms, dst_ref=mr.at[me], send_sem=m_ss.at[off - 1], recv_sem=m_rs.at[off - 1],
                                            device_id=(peer,), device_id_type=MESH)

    for off in far_first:
        m_send(off).start()
    mr[me] = ms[...]
    for off in range(1, ndev):
        m_send(off).wait_recv()
    m_tot = mr[0]
    for k in range(1, ndev):
        m_tot = m_tot + mr[k]
    m_out[...] = m_tot

    for s in range(ndev - 1):
        gb_send(s).wait_send()
    for off in range(1, ndev):
        ga_send(off).wait_send()
        m_send(off).wait_send()


def solve_kernel(tasks, m_ref, ga_in, gb_in, alpha_ref, ga_ref, gb_ref):
    m_all = m_ref[...]
    pairs = [(t, s) for t in range(tasks) for s in range(t, tasks)]
    gram = {pair: jnp.broadcast_to(m_all[:, p:p + 1], (8, 128)) for p, pair in enumerate(pairs)}
    trace = gram[0, 0]
    for t in range(1, tasks):
        trace = trace + gram[t, t]
    scale = trace / tasks
    gram = {pair: val / scale for pair, val in gram.items()}

    def eg_step(_, wts):
        new = []
        for t in range(tasks):
            acc = gram[0, t] * wts[0]
            for s in range(1, tasks):
                acc = acc + gram[min(t, s), max(t, s)] * wts[s]
            new.append(wts[t] * jnp.exp(-acc))
        tot = new[0]
        for t in range(1, tasks):
            tot = tot + new[t]
        inv = 1.0 / tot
        return tuple(w * inv for w in new)

    wts = lax.fori_loop(0, EG_STEPS, eg_step, tuple(jnp.full((8, 128), 1.0 / tasks, F32) for _ in range(tasks)), unroll=5)

    ga = wts[0] * ga_in[0:8]
    for t in range(1, tasks):
        ga = ga + wts[t] * ga_in[8 * t:8 * t + 8]
    ga_ref[...] = ga
    for k in range(gb_ref.shape[1] // 128):
        cols = slice(128 * k, 128 * (k + 1))
        gb = wts[0] * gb_in[0:8, cols]
        for t in range(1, tasks):
            gb = gb + wts[t] * gb_in[8 * t:8 * t + 8, cols]
        gb_ref[:, cols] = gb
    lane = lax.broadcasted_iota(jnp.int32, (8, 128), 1)
    alpha = wts[tasks - 1]
    for t in range(tasks - 1):
        alpha = jnp.where(lane == t, wts[t], alpha)
    alpha_ref[...] = alpha[0:1, 0:tasks]


def solution(mesh):
    num_dev = mesh.shape["data"]

    def device_step(tokens, labels, w_one, w_two, adapter_a, adapter_b, task_heads):
        tok, dm = tokens.shape
        rank, dff = adapter_b.shape
        tasks, _, ncls = task_heads.shape
        fb = dff // num_dev
        own = dm // num_dev
        prow = 8 * tasks + 8
        dma = pltpu.SemaphoreType.DMA
        hbm = pl.BlockSpec(memory_space=pltpu.HBM)
        vmem = pl.BlockSpec(memory_space=pltpu.VMEM)
        sums = pl.pallas_call(
            functools.partial(fused_kernel, num_dev, float(tok * num_dev)),
            name="fused_grads",
            out_shape=(jax.ShapeDtypeStruct((1, 128), F32), jax.ShapeDtypeStruct((8 * tasks, own), F32), jax.ShapeDtypeStruct((8 * tasks, fb), F32)),
            in_specs=[hbm] * 7,
            out_specs=(vmem, vmem, vmem),
            scratch_shapes=[
                pltpu.VMEM((tok, dm), BF16),
                pltpu.VMEM((num_dev, dm, fb), BF16),
                pltpu.VMEM((num_dev, fb, dm), BF16),
                pltpu.VMEM((rank, dm), BF16),
                pltpu.VMEM((rank, dff), BF16),
                pltpu.VMEM((tasks, ncls, dm), BF16),
                pltpu.VMEM((tasks, tok), jnp.int32),
                pltpu.VMEM((rank, tok), BF16),
                pltpu.VMEM((tok, rank), BF16),
                pltpu.VMEM((tok, fb), F32),
                pltpu.VMEM((tok, fb), F32),
                pltpu.VMEM((tok, fb), BF16),
                pltpu.VMEM((tok, fb), BF16),
                pltpu.VMEM((tok, fb), BF16),
                pltpu.VMEM((num_dev, fb, tok), F32),
                pltpu.VMEM((tok, dm), F32),
                pltpu.VMEM((prow, dm), BF16),
                pltpu.VMEM((dm, prow), BF16),
                pltpu.VMEM((tasks, dm, tok), BF16),
                pltpu.VMEM((tasks, fb, tok), BF16),
                pltpu.VMEM((tasks, fb, tok), BF16),
                pltpu.VMEM((prow, tok), F32),
                pltpu.VMEM((num_dev, 8 * tasks, fb), F32),
                pltpu.VMEM((num_dev - 1, 8 * tasks, fb), F32),
                pltpu.VMEM((num_dev, 8 * tasks, own), F32),
                pltpu.VMEM((num_dev - 1, 8 * tasks, own), F32),
                pltpu.VMEM((1, 128), F32),
                pltpu.VMEM((num_dev, 1, 128), F32),
                dma((num_dev,)),
                dma((num_dev,)),
                dma((5,)),
                dma((num_dev - 1,)),
                dma((num_dev - 1,)),
                dma((num_dev - 1,)),
                dma((num_dev - 1,)),
                dma((num_dev - 1,)),
                dma((num_dev - 1,)),
            ],
            compiler_params=pltpu.CompilerParams(collective_id=0, has_side_effects=True, vmem_limit_bytes=48 * 1024 * 1024),
        )(*[pltpu.with_memory_space_constraint(arr, pltpu.HBM) for arr in (tokens, labels, w_one, w_two, adapter_a.T, adapter_b, jnp.transpose(task_heads, (0, 2, 1)))])
        alpha, ga, gb = pl.pallas_call(
            functools.partial(solve_kernel, tasks),
            name="solve",
            out_shape=(jax.ShapeDtypeStruct((1, tasks), F32), jax.ShapeDtypeStruct((rank, own), F32), jax.ShapeDtypeStruct((rank, fb), F32)),
            in_specs=[vmem] * 3,
            out_specs=(vmem,) * 3,
            compiler_params=pltpu.CompilerParams(vmem_limit_bytes=2 * 1024 * 1024),
        )(*sums)
        return alpha.reshape(tasks), ga.T, gb

    return jax.shard_map(device_step, mesh=mesh, in_specs=(P("data", None), P(None, "data"), P(), P(), P(), P(), P()), out_specs=(P(), P("data", None), P(None, "data")), check_vma=False)
```

```python
import functools

import jax
import jax.numpy as jnp
import numpy as np
from jax import lax
from jax.experimental import pallas as pl
from jax.experimental.pallas import tpu as pltpu
from jax.sharding import PartitionSpec as P

EG_STEPS = 20
MESH = pl.DeviceIdType.MESH
F32, BF16 = jnp.float32, jnp.bfloat16
GELU_C = float(np.sqrt(2.0 / np.pi))
GELU_A = 0.044715
NT = (((1,), (1,)), ((), ()))


def dot(lhs, rhs):
    return jnp.dot(lhs, rhs, preferred_element_type=F32)


def dot_nt(lhs, rhs):
    return lax.dot_general(lhs, rhs, NT, preferred_element_type=F32)


def fused_kernel(ndev, batch_total, x_hbm, lab_hbm, w1_hbm, w2_hbm, at_hbm, bm_hbm, ht_hbm,
                 m_out, ga_out, gb_out,
                 xs, w1s, w2s, ats, bms, hts_in, labs, uts, us, p_a, p_b, h_a, h_b, h_c, slope, zacc,
                 hrow, hcol, dzs, dp_a, dp_b, dlacc, gbs, gbr, gas, gar, ms, mr,
                 w1sem, w2sem, insem, gb_ss, gb_rs, ga_ss, ga_rs, m_ss, m_rs):
    tok = xs.shape[0]
    dff = w2_hbm.shape[0]
    fb = dff // ndev
    rank = ats.shape[0]
    tasks = hts_in.shape[0]
    ncls = hts_in.shape[1]
    dm = xs.shape[1]
    own = dm // ndev
    me = lax.axis_index("data")

    def peer_of(flip):
        b, w = 0, 1
        while w < ndev:
            b = b + w * lax.rem(me // w + flip // w, 2)
            w *= 2
        return b

    far_first = range(ndev - 1, 0, -1)

    def small(i):
        pairs = [(at_hbm, ats), (x_hbm, xs), (bm_hbm, bms), (ht_hbm, hts_in), (lab_hbm, labs)]
        return pltpu.make_async_copy(pairs[i][0], pairs[i][1], insem.at[i])

    def w1_copy(j):
        return pltpu.make_async_copy(w1_hbm.at[:, pl.ds(pl.multiple_of(j * fb, fb), fb)], w1s.at[j], w1sem.at[j])

    def w2_copy(j):
        return pltpu.make_async_copy(w2_hbm.at[pl.ds(pl.multiple_of(j * fb, fb), fb), :], w2s.at[j], w2sem.at[j])

    for i in (1, 0, 3):
        small(i).start()
    w1_copy(0).start()
    w1_copy(1).start()
    small(2).start()
    small(4).start()
    w2_copy(0).start()
    for j in range(2, ndev):
        w1_copy(j).start()
        w2_copy(j - 1).start()
    w2_copy(ndev - 1).start()

    barrier = pltpu.get_barrier_semaphore()
    for flip in far_first:
        pl.semaphore_signal(barrier, inc=1, device_id=(peer_of(flip),), device_id_type=MESH)

    zacc[...] = jnp.zeros_like(zacc)
    dlacc[...] = jnp.zeros_like(dlacc)
    small(3).wait()
    pad = jnp.zeros((8 - ncls, dm), F32)
    heads = []
    for t in range(tasks):
        heads += [hts_in[t].astype(F32), pad]
    heads = jnp.concatenate(heads + [jnp.zeros((8, dm), F32)], axis=0)
    hrow[...] = heads.astype(BF16)
    hcol[...] = heads.T.astype(BF16)

    small(0).wait()
    small(1).wait()
    ut = dot_nt(ats[...], xs[...])
    uts[...] = ut.astype(BF16)
    us[...] = ut.T.astype(BF16)
    small(2).wait()
    small(4).wait()
    w1_copy(0).wait()
    w1_copy(1).wait()

    def block_of(ref, j):
        return ref[:, pl.ds(pl.multiple_of(j * fb, fb), fb)]

    half, quarter = tok // 2, tok // 4

    def fwd_in(j, p_ref, i):
        rows = slice(half * i, half * (i + 1))
        p_ref[rows] = dot(xs[rows], w1s[j]) + dot(us[rows], block_of(bms, j))

    def fwd_act(j, p_ref, h_ref, i):
        rows = slice(quarter * i, quarter * (i + 1))
        x = p_ref[rows]
        x2 = x * x
        t = jnp.tanh(x * (GELU_C + (GELU_C * GELU_A) * x2))
        cdf = 0.5 + 0.5 * t
        h_ref[rows] = (x * cdf).astype(BF16)
        w = cdf * (1.0 - cdf)
        slope[j, :, rows] = (cdf + x * (w * (2.0 * GELU_C + (6.0 * GELU_C * GELU_A) * x2))).T

    def fwd_out(j, h_ref):
        zacc[...] += dot(h_ref[...], w2s[j])

    ps, hs = (p_a, p_b), (h_a, h_b, h_c)
    for i in range(2):
        fwd_in(0, p_a, i)
    for i in range(2):
        fwd_in(1, p_b, i)
        fwd_act(0, p_a, h_a, 2 * i)
        fwd_act(0, p_a, h_a, 2 * i + 1)

    def fwd_pair(i, carry):
        for k in range(2):
            w1_copy(2 * i + k + 2).wait()
            w2_copy(2 * i + k).wait()
        for k in range(2):
            j = 2 * i + k
            for q in range(4):
                if q < 2:
                    fwd_in(j + 2, ps[k], q)
                fwd_act(j + 1, ps[1 - k], hs[1 + k], q)
        zacc[...] += dot(h_a[...], w2s[2 * i]) + dot(h_b[...], w2s[2 * i + 1])
        h_a[...] = h_c[...]
        return carry

    lax.fori_loop(0, (ndev - 2) // 2, fwd_pair, 0)
    pl.semaphore_wait(barrier, ndev - 1)
    w2_copy(ndev - 2).wait()
    w2_copy(ndev - 1).wait()
    fwd_out(ndev - 2, h_a)
    for i in range(2):
        fwd_act(ndev - 1, p_b, h_b, 2 * i)
        fwd_act(ndev - 1, p_b, h_b, 2 * i + 1)
    cls = lax.broadcasted_iota(jnp.int32, (8, half), 0)
    z = (xs[...].astype(F32) + (zacc[...] + dot(h_b[...], w2s[ndev - 1]))).astype(BF16)
    both = dot_nt(hrow[...], z)
    logits = [both[:, :half], both[:, half:]]
    errs = [[] for _ in range(tasks)]
    for i in range(2):
        rows = slice(half * i, half * (i + 1))
        for t in range(tasks):
            lg = jnp.where(cls < ncls, logits[i][8 * t:8 * t + 8], -jnp.inf)
            e = jnp.exp(lg - jnp.max(lg, axis=0, keepdims=True))
            prob = e / jnp.sum(e, axis=0, keepdims=True)
            errs[t].append(prob - (cls == labs[t:t + 1, rows]).astype(F32))
    blank = jnp.zeros((8, tok), F32)
    for t in range(tasks):
        err = jnp.concatenate([jnp.concatenate(errs[t], axis=1) if k == t else blank for k in range(tasks + 1)], axis=0)
        dzs[t] = dot(hcol[...], err.astype(BF16)).astype(BF16)


    def blk(s):
        return peer_of(ndev - 1 - s)

    def low_piece(s, dp_ref, t, i):
        part = slice(fb // 2 * i, fb // 2 * (i + 1))
        return dot(block_of(bms, blk(s))[:, part], dp_ref[t, part, :])

    def col_piece(dp_ref, t, i):
        part = slice(tok // 2 * i, tok // 2 * (i + 1))
        return dot_nt(uts[:, part], dp_ref[t, :, part])

    def bwd_step(s, dp_new, dp_old, cols=True):
        b = blk(s)
        for t in range(tasks):
            dh, low, col = None, [], []
            for q in range(4):
                part = slice(dm // 4 * q, dm // 4 * (q + 1))
                piece = dot(w2s[b, :, part], dzs[t, part, :])
                dh = piece if dh is None else dh + piece
                if dp_old is not None and q % 2 == 0:
                    if cols:
                        col.append(col_piece(dp_old, t, q // 2))
                    low.append(low_piece(s - 1, dp_old, t, q // 2))
            dp_new[t] = (dh * slope[b]).astype(BF16)
            if low:
                dlacc[8 * t:8 * t + 8] += low[0] + low[1]
            if col:
                gbs[s - 1, 8 * t:8 * t + 8] = col[0] + col[1]

    def bwd_low(s, dp_ref):
        for t in range(tasks):
            dlacc[8 * t:8 * t + 8] += low_piece(s, dp_ref, t, 0) + low_piece(s, dp_ref, t, 1)

    def bwd_col(s, dp_ref):
        for t in range(tasks):
            gbs[s, 8 * t:8 * t + 8] = col_piece(dp_ref, t, 0) + col_piece(dp_ref, t, 1)

    def gb_send(s):
        return pltpu.make_async_remote_copy(src_ref=gbs.at[s], dst_ref=gbr.at[s], send_sem=gb_ss.at[s], recv_sem=gb_rs.at[s],
                                            device_id=(blk(s),), device_id_type=MESH)

    dps = (dp_a, dp_b)
    bwd_step(0, dp_a, None)

    def bwd_pair(i, carry):
        for k in range(2):
            bwd_step(2 * i + k + 1, dps[1 - k], dps[k])
        for k in range(2):
            gb_send(2 * i + k).start()
        return carry

    lax.fori_loop(0, (ndev - 2) // 2, bwd_pair, 0)
    bwd_step(ndev - 1, dp_b, dp_a, cols=False)
    bwd_low(ndev - 1, dp_b)

    ga_t = dot(dlacc[...].astype(BF16), xs[...])
    for k in range(ndev):
        gas[k] = ga_t[:8 * tasks, own * k:own * (k + 1)]

    def ga_send(off):
        peer = peer_of(off)
        return pltpu.make_async_remote_copy(src_ref=gas.at[peer], dst_ref=gar.at[off - 1], send_sem=ga_ss.at[off - 1], recv_sem=ga_rs.at[off - 1],
                                            device_id=(peer,), device_id_type=MESH)

    for off in far_first:
        ga_send(off).start()

    bwd_col(ndev - 2, dp_a)
    gb_send(ndev - 2).start()
    bwd_col(ndev - 1, dp_b)
    gb_sum = gbs[ndev - 1]
    for s in range(ndev - 1):
        gb_send(s).wait_recv()
        gb_sum = gb_sum + gbr[s]
    gb_sum = gb_sum * (1.0 / batch_total)
    gb_out[...] = gb_sum

    pairs = [(t, s) for t in range(tasks) for s in range(t, tasks)]
    gram_b = []
    for t, s in pairs:
        prod = gb_sum[8 * t:8 * t + 8] * gb_sum[8 * s:8 * s + 8]
        tot = prod[:, 0:128]
        for k in range(1, fb // 128):
            tot = tot + prod[:, 128 * k:128 * (k + 1)]
        gram_b.append(tot)

    ga_sum = gas[me]
    for off in range(1, ndev):
        ga_send(off).wait_recv()
        ga_sum = ga_sum + gar[off - 1]
    ga_sum = ga_sum * (1.0 / batch_total)
    ga_out[...] = ga_sum

    rows = []
    for p, (t, s) in enumerate(pairs):
        prod = ga_sum[8 * t:8 * t + 8] * ga_sum[8 * s:8 * s + 8] + gram_b[p]
        rows.append(jnp.sum(prod, axis=0, keepdims=True))
    lane = lax.broadcasted_iota(jnp.int32, (1, 128), 1)
    m_own = jnp.zeros((1, 128), F32)
    for p, row in enumerate(rows):
        m_own = jnp.where(lane == p, jnp.sum(row, axis=1, keepdims=True), m_own)
    ms[...] = m_own

    def m_send(off):
        peer = peer_of(off)
        return pltpu.make_async_remote_copy(src_ref=ms, dst_ref=mr.at[me], send_sem=m_ss.at[off - 1], recv_sem=m_rs.at[off - 1],
                                            device_id=(peer,), device_id_type=MESH)

    for off in far_first:
        m_send(off).start()
    mr[me] = ms[...]
    for off in range(1, ndev):
        m_send(off).wait_recv()
    m_tot = mr[0]
    for k in range(1, ndev):
        m_tot = m_tot + mr[k]
    m_out[...] = m_tot

    for s in range(ndev - 1):
        gb_send(s).wait_send()
    for off in range(1, ndev):
        ga_send(off).wait_send()
        m_send(off).wait_send()


def solve_kernel(tasks, m_ref, ga_in, gb_in, alpha_ref, ga_ref, gb_ref):
    m_all = m_ref[...]
    pairs = [(t, s) for t in range(tasks) for s in range(t, tasks)]
    gram = {pair: jnp.broadcast_to(m_all[:, p:p + 1], (8, 128)) for p, pair in enumerate(pairs)}
    trace = gram[0, 0]
    for t in range(1, tasks):
        trace = trace + gram[t, t]
    scale = trace / tasks
    gram = {pair: val / scale for pair, val in gram.items()}

    def eg_step(_, wts):
        new = []
        for t in range(tasks):
            acc = gram[0, t] * wts[0]
            for s in range(1, tasks):
                acc = acc + gram[min(t, s), max(t, s)] * wts[s]
            new.append(wts[t] * jnp.exp(-acc))
        tot = new[0]
        for t in range(1, tasks):
            tot = tot + new[t]
        inv = 1.0 / tot
        return tuple(w * inv for w in new)

    wts = lax.fori_loop(0, EG_STEPS, eg_step, tuple(jnp.full((8, 128), 1.0 / tasks, F32) for _ in range(tasks)), unroll=EG_STEPS)

    ga = wts[0] * ga_in[0:8]
    for t in range(1, tasks):
        ga = ga + wts[t] * ga_in[8 * t:8 * t + 8]
    ga_ref[...] = ga
    for k in range(gb_ref.shape[1] // 128):
        cols = slice(128 * k, 128 * (k + 1))
        gb = wts[0] * gb_in[0:8, cols]
        for t in range(1, tasks):
            gb = gb + wts[t] * gb_in[8 * t:8 * t + 8, cols]
        gb_ref[:, cols] = gb
    lane = lax.broadcasted_iota(jnp.int32, (8, 128), 1)
    alpha = wts[tasks - 1]
    for t in range(tasks - 1):
        alpha = jnp.where(lane == t, wts[t], alpha)
    alpha_ref[...] = alpha[0:1, 0:tasks]


def solution(mesh):
    num_dev = mesh.shape["data"]

    def device_step(tokens, labels, w_one, w_two, adapter_a, adapter_b, task_heads):
        tok, dm = tokens.shape
        rank, dff = adapter_b.shape
        tasks, _, ncls = task_heads.shape
        fb = dff // num_dev
        own = dm // num_dev
        prow = 8 * tasks + 8
        dma = pltpu.SemaphoreType.DMA
        hbm = pl.BlockSpec(memory_space=pltpu.HBM)
        vmem = pl.BlockSpec(memory_space=pltpu.VMEM)
        sums = pl.pallas_call(
            functools.partial(fused_kernel, num_dev, float(tok * num_dev)),
            name="fused_grads",
            out_shape=(jax.ShapeDtypeStruct((1, 128), F32), jax.ShapeDtypeStruct((8 * tasks, own), F32), jax.ShapeDtypeStruct((8 * tasks, fb), F32)),
            in_specs=[hbm] * 7,
            out_specs=(vmem, vmem, vmem),
            scratch_shapes=[
                pltpu.VMEM((tok, dm), BF16),
                pltpu.VMEM((num_dev, dm, fb), BF16),
                pltpu.VMEM((num_dev, fb, dm), BF16),
                pltpu.VMEM((rank, dm), BF16),
                pltpu.VMEM((rank, dff), BF16),
                pltpu.VMEM((tasks, ncls, dm), BF16),
                pltpu.VMEM((tasks, tok), jnp.int32),
                pltpu.VMEM((rank, tok), BF16),
                pltpu.VMEM((tok, rank), BF16),
                pltpu.VMEM((tok, fb), F32),
                pltpu.VMEM((tok, fb), F32),
                pltpu.VMEM((tok, fb), BF16),
                pltpu.VMEM((tok, fb), BF16),
                pltpu.VMEM((tok, fb), BF16),
                pltpu.VMEM((num_dev, fb, tok), F32),
                pltpu.VMEM((tok, dm), F32),
                pltpu.VMEM((prow, dm), BF16),
                pltpu.VMEM((dm, prow), BF16),
                pltpu.VMEM((tasks, dm, tok), BF16),
                pltpu.VMEM((tasks, fb, tok), BF16),
                pltpu.VMEM((tasks, fb, tok), BF16),
                pltpu.VMEM((prow, tok), F32),
                pltpu.VMEM((num_dev, 8 * tasks, fb), F32),
                pltpu.VMEM((num_dev - 1, 8 * tasks, fb), F32),
                pltpu.VMEM((num_dev, 8 * tasks, own), F32),
                pltpu.VMEM((num_dev - 1, 8 * tasks, own), F32),
                pltpu.VMEM((1, 128), F32),
                pltpu.VMEM((num_dev, 1, 128), F32),
                dma((num_dev,)),
                dma((num_dev,)),
                dma((5,)),
                dma((num_dev - 1,)),
                dma((num_dev - 1,)),
                dma((num_dev - 1,)),
                dma((num_dev - 1,)),
                dma((num_dev - 1,)),
                dma((num_dev - 1,)),
            ],
            compiler_params=pltpu.CompilerParams(collective_id=0, has_side_effects=True, vmem_limit_bytes=48 * 1024 * 1024),
        )(*[pltpu.with_memory_space_constraint(arr, pltpu.HBM) for arr in (tokens, labels, w_one, w_two, adapter_a.T, adapter_b, jnp.transpose(task_heads, (0, 2, 1)))])
        alpha, ga, gb = pl.pallas_call(
            functools.partial(solve_kernel, tasks),
            name="solve",
            out_shape=(jax.ShapeDtypeStruct((1, tasks), F32), jax.ShapeDtypeStruct((rank, own), F32), jax.ShapeDtypeStruct((rank, fb), F32)),
            in_specs=[vmem] * 3,
            out_specs=(vmem,) * 3,
            compiler_params=pltpu.CompilerParams(vmem_limit_bytes=2 * 1024 * 1024),
        )(*sums)
        return alpha.reshape(tasks), ga.T, gb

    return jax.shard_map(device_step, mesh=mesh, in_specs=(P("data", None), P(None, "data"), P(), P(), P(), P(), P()), out_specs=(P(), P("data", None), P(None, "data")), check_vma=False)
```
